32 devices in a mesh: gy: 4 (over z), gx: 8 (over y, x, core).
Axes of the slice: x: 2, y: 2, z: 4, core: 2. Of those that a mesh axis runs over, the one named last changes fastest.
Arguments:
- coefficients: float32 [9, 128, 256], P(None, 'gy', 'gx'), may hold values from -2.1 to 2.1
- vectors: float32 [128, 256, 2048], P('gy', 'gx'), may hold values from -6 to 6
Outputs:
- normal: float32 [25, 128, 256], P(None, 'gy', 'gx')
- image: float32 [128, 256, 2048], P('gy', 'gx')
The draws below stay inside these ranges and needn't reach their ends.
All inputs are finite; a program needn't handle non-finite values.
Results may differ from the reference program's by a relative error of at most 0.00002.
Values sent between devices are 32-bit elements; how exact they have to be, the bound alone decides.
No kernel may reach another device: no remote copies, remote signals or barrier semaphores. Data moves between devices by JAX's collectives and lax.ppermute only.
A program may use at most 192 MiB of HBM per device.

```python
import math
import jax
import jax.numpy as jnp
from jax import lax

NV = 2048
NX = 128
NY = 256


def block_levels(rng, shape, shards, least, largest):
    def one(axis_at, parts):
        heights = jax.random.uniform(jax.random.fold_in(jax.random.fold_in(rng, 6), axis_at), (parts,), jnp.float32, least / len(shards), largest / len(shards))
        return jnp.repeat(jnp.exp(heights), shape[axis_at] // parts).reshape((-1,) + (1,) * (len(shape) - axis_at - 1))

    loudness = one(*shards[0])
    for cut in shards[1:]:
        loudness = loudness * one(*cut)
    return loudness


def centred(stream_key, shape, spread, limit, cuts=(), held_as=jnp.bfloat16):
    gain = block_levels(stream_key, shape, cuts, -0.22, 0.18) if cuts else 1.0
    drawn = jax.random.normal(stream_key, shape, jnp.float32) * spread * gain
    return jnp.minimum(jnp.maximum(drawn, -limit), limit).astype(held_as)


def setup_inputs(seed: int = 0) -> dict:
    keys = jax.random.split(jax.random.key(seed), 3)
    coefficients = centred(keys[0], (9, NX, NY), 0.35, 2.1, ((1, 4), (2, 8)), jnp.float32)
    vectors = centred(keys[1], (NX, NY, NV), 1.0, 6.0, ((0, 4), (1, 8)), jnp.float32)
    return dict(coefficients=coefficients, vectors=vectors)


def reference(coefficients, vectors):
    row_pos = jnp.arange(NX, dtype=jnp.int32)[:, None]
    col_pos = jnp.arange(NY, dtype=jnp.int32)[None, :]
    pieces = []
    for k in range(9):
        a = k // 3 - 1
        b = k % 3 - 1
        inside = (row_pos + a >= 0) & (row_pos + a < NX) & (col_pos + b >= 0) & (col_pos + b < NY)
        pieces.append(jnp.where(inside, coefficients[k], jnp.zeros_like(coefficients[k])))
    masked = jnp.stack(pieces)
    padded = jnp.pad(masked, ((0, 0), (1, 1), (1, 1)))
    terms = [jnp.zeros((NX, NY), coefficients.dtype) for slot in range(25)]
    for k in range(9):
        a = k // 3 - 1
        b = k % 3 - 1
        for m in range(9):
            e = (m // 3) - (k // 3)
            f = (m % 3) - (k % 3)
            slot_index = (e + 2) * 5 + (f + 2)
            first = padded[k, 1 - a:1 - a + NX, 1 - b:1 - b + NY]
            second = padded[m, 1 - a:1 - a + NX, 1 - b:1 - b + NY]
            terms[slot_index] = terms[slot_index] + first * second
    normal = jnp.stack(terms)
    block = math.gcd(NV, 128)

    def one_block(step, image):
        part = lax.dynamic_slice_in_dim(vectors, step * block, block, 2)
        wide = jnp.pad(part, ((2, 2), (2, 2), (0, 0)))
        total = jnp.zeros((NX, NY, block), vectors.dtype)
        for e in range(-2, 3):
            for f in range(-2, 3):
                slot_index = (e + 2) * 5 + (f + 2)
                total = total + normal[slot_index][:, :, None] * wide[2 + e:2 + e + NX, 2 + f:2 + f + NY, :]
        return lax.dynamic_update_slice_in_dim(image, total, step * block, 2)

    image = lax.fori_loop(0, NV // block, one_block, jnp.zeros_like(vectors))
    return normal, image
```

```python
import jax
import jax.numpy as jnp
import numpy as np
from jax import lax
from jax.experimental import pallas as pl
from jax.experimental.pallas import tpu as pltpu
from jax.sharding import PartitionSpec as P


GROUP = 2


def shift_up(block, axis):
    n = lax.axis_size(axis)
    return lax.ppermute(block, axis, [(i, i + 1) for i in range(n - 1)])


def shift_down(block, axis):
    n = lax.axis_size(axis)
    return lax.ppermute(block, axis, [(i + 1, i) for i in range(n - 1)])


def masked_weights(coefficients):
    _, rows, cols = coefficients.shape
    total_rows = rows * lax.axis_size("gy")
    total_cols = cols * lax.axis_size("gx")
    k = jnp.arange(9, dtype=jnp.int32)[:, None, None]
    r = lax.axis_index("gy") * rows + jnp.arange(rows, dtype=jnp.int32)[None, :, None] + k // 3 - 1
    c = lax.axis_index("gx") * cols + jnp.arange(cols, dtype=jnp.int32)[None, None, :] + k % 3 - 1
    inside = (r >= 0) & (r < total_rows) & (c >= 0) & (c < total_cols)
    return jnp.where(inside, coefficients, 0.0)


def normal_kernel(ext_ref, out_ref):
    _, rows, cols = out_ref.shape
    acc = {}
    for k in range(9):
        a, b = k // 3 - 1, k % 3 - 1
        cells = [ext_ref[m, 1 - a : 1 - a + rows, 1 - b : 1 - b + cols] for m in range(9)]
        for m in range(9):
            slot = (m // 3 - k // 3 + 2) * 5 + (m % 3 - k % 3 + 2)
            product = cells[k] * cells[m]
            acc[slot] = acc[slot] + product if slot in acc else product
    for slot in range(25):
        out_ref[slot] = acc[slot]


def split(x):
    hi = x.astype(jnp.bfloat16)
    lo = (x - hi.astype(jnp.float32)).astype(jnp.bfloat16)
    return hi, lo


def image_kernel(rows, cols, pitch, depth):
    m = GROUP * cols

    def body(n_ref, t_ref, x_ref, top_ref, bot_ref, left_ref, right_ref, cl_ref, cr_ref, out_ref, w_ref, u_ref, hi_ref, lo_ref):
        lanes = x_ref.shape[1]

        @pl.when(pl.program_id(0) == 0)
        def _():
            n_hi, n_lo = split(n_ref[...])
            dims = (((0,), (0,)), ((), ()))
            u_ref[...] = lax.dot_general(n_hi, t_ref[...], dims, preferred_element_type=jnp.float32) + lax.dot_general(
                n_lo, t_ref[...], dims, preferred_element_type=jnp.float32
            )
            for r in range(rows):
                g, ro = divmod(r, GROUP)
                band = pltpu.roll(u_ref[r * cols : (r + 1) * cols, :], ro * pitch, 1, stride=1, stride_axis=0)
                hi, lo = split(band)
                w_ref[g, ro * cols : (ro + 1) * cols, :] = hi
                w_ref[g, m + ro * cols : m + (ro + 1) * cols, :] = lo

        pad = jnp.zeros((pitch - cols - 4, lanes), jnp.float32)

        def wide_row(i):
            if i < 2:
                mid, l, r = top_ref[i * cols : (i + 1) * cols, :], cl_ref[i], cr_ref[i]
            elif i < rows + 2:
                q = i - 2
                mid, l, r = x_ref[q * cols : (q + 1) * cols, :], left_ref[q], right_ref[q]
            else:
                q = i - rows - 2
                mid, l, r = bot_ref[q * cols : (q + 1) * cols, :], cl_ref[q + 2], cr_ref[q + 2]
            return [l, mid, r, pad]

        for i in range(0, rows + 4, 2):
            pair = jnp.concatenate(wide_row(i) + wide_row(i + 1), axis=0)
            hi, lo = split(pair)
            hi_ref[i * pitch : (i + 2) * pitch, :] = hi
            lo_ref[i * pitch : (i + 2) * pitch, :] = lo
        tail = hi_ref.shape[0] - (rows + 4) * pitch
        if tail:
            hi_ref[(rows + 4) * pitch :, :] = jnp.zeros((tail, lanes), jnp.bfloat16)
            lo_ref[(rows + 4) * pitch :, :] = jnp.zeros((tail, lanes), jnp.bfloat16)
        for g in range(rows // GROUP):
            at = g * GROUP * pitch
            first = jnp.dot(w_ref[g], hi_ref[at : at + depth, :], preferred_element_type=jnp.float32)
            second = jnp.dot(w_ref[g, :m, :], lo_ref[at : at + depth, :], preferred_element_type=jnp.float32)
            out_ref[g * m : (g + 1) * m, :] = first[:m] + (first[m:] + second)

    return body


def per_device(coefficients, vectors):
    _, rows, cols = coefficients.shape
    nv = vectors.shape[2]
    left = shift_up(vectors[:, cols - 2 :, :], "gx")
    right = shift_down(vectors[:, :2, :], "gx")
    top = shift_up(vectors[rows - 2 :], "gy")
    bot = shift_down(vectors[:2], "gy")
    masked = masked_weights(coefficients)
    ext = jnp.concatenate([shift_up(masked[:, rows - 1 :, :], "gy"), masked, shift_down(masked[:, :1, :], "gy")], axis=1)
    ext = jnp.concatenate([shift_up(ext[:, :, cols - 1 :], "gx"), ext, shift_down(ext[:, :, :1], "gx")], axis=2)
    normal = pl.pallas_call(normal_kernel, out_shape=jax.ShapeDtypeStruct((25, rows, cols), jnp.float32), name="normal")(ext)
    ends = jnp.concatenate([top, bot], axis=0)
    cl = shift_up(ends[:, cols - 2 :, :], "gx")
    cr = shift_down(ends[:, :2, :], "gx")

    pitch = -(-(cols + 4) // 8) * 8
    depth = -(-((GROUP + 4) * pitch) // 128) * 128
    spread = np.zeros((32, depth), np.float32)
    for s in range(25):
        spread[s, (s // 5) * pitch + s % 5] = 1.0
    flat = jnp.pad(normal.reshape(25, rows * cols), ((0, 7), (0, 0)))
    lanes = min(nv, 256)
    wide_rows = (rows - GROUP) * pitch + depth
    wide_rows = -(-max(wide_rows, (rows + 4) * pitch) // 16) * 16
    m = GROUP * cols
    fixed = lambda *s: pl.BlockSpec(s, lambda j: (0,) * len(s))
    flat_block = lambda n: pl.BlockSpec((n, lanes), lambda j: (0, j))
    edge_block = lambda n: pl.BlockSpec((n, 2, lanes), lambda j: (0, 0, j))
    image = pl.pallas_call(
        image_kernel(rows, cols, pitch, depth),
        grid=(nv // lanes,),
        in_specs=[
            fixed(32, rows * cols),
            fixed(32, depth),
            flat_block(rows * cols),
            flat_block(2 * cols),
            flat_block(2 * cols),
            edge_block(rows),
            edge_block(rows),
            edge_block(4),
            edge_block(4),
        ],
        out_specs=flat_block(rows * cols),
        out_shape=jax.ShapeDtypeStruct((rows * cols, nv), jnp.float32),
        scratch_shapes=[
            pltpu.VMEM((rows // GROUP, 2 * m, depth), jnp.bfloat16),
            pltpu.VMEM((rows * cols, depth), jnp.float32),
            pltpu.VMEM((wide_rows, lanes), jnp.bfloat16),
            pltpu.VMEM((wide_rows, lanes), jnp.bfloat16),
        ],
        compiler_params=pltpu.CompilerParams(dimension_semantics=("arbitrary",)),
        name="image",
    )(
        flat,
        jnp.asarray(spread, jnp.bfloat16),
        vectors.reshape(rows * cols, nv),
        top.reshape(2 * cols, nv),
        bot.reshape(2 * cols, nv),
        left,
        right,
        cl,
        cr,
    )
    return normal, image.reshape(rows, cols, nv)


def solution(mesh):
    in_specs = (P(None, "gy", "gx"), P("gy", "gx", None))
    out_specs = (P(None, "gy", "gx"), P("gy", "gx", None))
    return jax.shard_map(per_device, mesh=mesh, in_specs=in_specs, out_specs=out_specs, check_vma=False)
```

```python
import jax
import jax.numpy as jnp
import numpy as np
from jax import lax
from jax.experimental import pallas as pl
from jax.experimental.pallas import tpu as pltpu
from jax.sharding import PartitionSpec as P


GROUP = 2


def inner_swap(block, axis):
    n = lax.axis_size(axis)
    return lax.ppermute(block, axis, [(i, i ^ 1) for i in range(n) if i ^ 1 < n])


def outer_swap(block, axis):
    n = lax.axis_size(axis)
    partner = {i: ((i + 1) ^ 1) - 1 for i in range(n)}
    return lax.ppermute(block, axis, [(i, p) for i, p in partner.items() if 0 <= p < n])


def masked_weights(coefficients):
    _, rows, cols = coefficients.shape
    total_rows = rows * lax.axis_size("gy")
    total_cols = cols * lax.axis_size("gx")
    k = jnp.arange(9, dtype=jnp.int32)[:, None, None]
    r = lax.axis_index("gy") * rows + jnp.arange(rows, dtype=jnp.int32)[None, :, None] + k // 3 - 1
    c = lax.axis_index("gx") * cols + jnp.arange(cols, dtype=jnp.int32)[None, None, :] + k % 3 - 1
    inside = (r >= 0) & (r < total_rows) & (c >= 0) & (c < total_cols)
    return jnp.where(inside, coefficients, 0.0)


def normal_terms(ext_ref, rows, cols):
    acc = {}
    for k in range(9):
        a, b = k // 3 - 1, k % 3 - 1
        cells = [ext_ref[m, 1 - a : 1 - a + rows, 1 - b : 1 - b + cols] for m in range(9)]
        for m in range(9):
            slot = (m // 3 - k // 3 + 2) * 5 + (m % 3 - k % 3 + 2)
            product = cells[k] * cells[m]
            acc[slot] = acc[slot] + product if slot in acc else product
    return acc


def split(x):
    hi = x.astype(jnp.bfloat16)
    lo = (x - hi.astype(jnp.float32)).astype(jnp.bfloat16)
    return hi, lo


def image_kernel(rows, cols, pitch, depth):
    m = GROUP * cols

    def body(odd_ref, ext_ref, t_ref, x_ref, rin_ref, rout_ref, cin_ref, cout_ref, kin_ref, kout_ref, n_ref, out_ref, w_ref, n2_ref, hi_ref, lo_ref):
        lanes = x_ref.shape[1]
        odd_y = odd_ref[0] == 1
        odd_x = odd_ref[1] == 1

        @pl.when(pl.program_id(0) == 0)
        def _():
            for slot, term in normal_terms(ext_ref, rows, cols).items():
                n_ref[slot] = term
                n2_ref[:, slot, :] = term
            n2_ref[:, 25:, :] = jnp.zeros((rows, n2_ref.shape[1] - 25, cols), jnp.float32)
            dims = (((0,), (0,)), ((), ()))
            for r in range(rows):
                g, ro = divmod(r, GROUP)
                n_hi, n_lo = split(n2_ref[r])
                band = lax.dot_general(n_hi, t_ref[...], dims, preferred_element_type=jnp.float32) + lax.dot_general(
                    n_lo, t_ref[...], dims, preferred_element_type=jnp.float32
                )
                band = pltpu.roll(band, ro * pitch, 1, stride=1, stride_axis=0)
                hi, lo = split(band)
                w_ref[g, ro * cols : (ro + 1) * cols, :] = hi
                w_ref[g, m + ro * cols : m + (ro + 1) * cols, :] = lo

        pad = jnp.zeros((pitch - cols - 4, lanes), jnp.float32)

        def sides(near_ref, far_ref, q):
            near, far = near_ref[q], far_ref[q]
            return jnp.where(odd_x, near, far), jnp.where(odd_x, far, near)

        def wide_row(i):
            if i < 2:
                at = slice(i * cols, (i + 1) * cols)
                mid = jnp.where(odd_y, rin_ref[at, :], rout_ref[at, :])
                l, r = sides(kin_ref, kout_ref, i)
            elif i < rows + 2:
                q = i - 2
                mid = x_ref[q * cols : (q + 1) * cols, :]
                l, r = sides(cin_ref, cout_ref, q)
            else:
                q = i - rows - 2
                at = slice(q * cols, (q + 1) * cols)
                mid = jnp.where(odd_y, rout_ref[at, :], rin_ref[at, :])
                l, r = sides(kin_ref, kout_ref, q + 2)
            return [l, mid, r, pad]

        for i in range(0, rows + 4, 2):
            pair = jnp.concatenate(wide_row(i) + wide_row(i + 1), axis=0)
            hi, lo = split(pair)
            hi_ref[i * pitch : (i + 2) * pitch, :] = hi
            lo_ref[i * pitch : (i + 2) * pitch, :] = lo
        tail = hi_ref.shape[0] - (rows + 4) * pitch
        if tail:
            hi_ref[(rows + 4) * pitch :, :] = jnp.zeros((tail, lanes), jnp.bfloat16)
            lo_ref[(rows + 4) * pitch :, :] = jnp.zeros((tail, lanes), jnp.bfloat16)
        for g in range(rows // GROUP):
            at = g * GROUP * pitch
            first = jnp.dot(w_ref[g], hi_ref[at : at + depth, :], preferred_element_type=jnp.float32)
            second = jnp.dot(w_ref[g, :m, :], lo_ref[at : at + depth, :], preferred_element_type=jnp.float32)
            out_ref[g * m : (g + 1) * m, :] = first[:m] + (first[m:] + second)

    return body


def edges(cells, odd, dim, width):
    size = cells.shape[dim]
    last = lax.slice_in_dim(cells, size - width, size, axis=dim)
    first = lax.slice_in_dim(cells, 0, width, axis=dim)
    return jnp.where(odd, first, last), jnp.where(odd, last, first)


def swapped(pair, axis):
    outer = outer_swap(pair[1], axis)
    return inner_swap(pair[0], axis), outer


def per_device(coefficients, vectors):
    _, rows, cols = coefficients.shape
    nv = vectors.shape[2]
    odd_y = lax.axis_index("gy") % 2
    odd_x = lax.axis_index("gx") % 2
    oy, ox = odd_y == 1, odd_x == 1
    cin, cout = swapped(edges(vectors, ox, 1, 2), "gx")
    row_last = lax.dynamic_slice_in_dim(vectors, jnp.where(oy, 0, rows - 2), 2, axis=0)
    row_first = lax.dynamic_slice_in_dim(vectors, jnp.where(oy, rows - 2, 0), 2, axis=0)
    rin, rout = swapped((row_last, row_first), "gy")
    masked = masked_weights(coefficients)
    min_, mout = swapped(edges(masked, oy, 1, 1), "gy")
    ext = jnp.concatenate([jnp.where(oy, min_, mout), masked, jnp.where(oy, mout, min_)], axis=1)
    corner = []
    for vin, vout, w in zip(edges(rin, ox, 1, 2), edges(rout, ox, 1, 2), edges(ext, ox, 2, 1)):
        extra = 2 * nv * (-(-w.size // (2 * nv)))
        w = jnp.pad(w.reshape(-1), (0, extra - w.size)).reshape(-1, 2, nv)
        corner.append(jnp.concatenate([jnp.where(oy, vin, vout), jnp.where(oy, vout, vin), w], axis=0))
    kin, kout = swapped(corner, "gx")
    win, wout = [k[4:].reshape(-1)[: 9 * (rows + 2)].reshape(9, rows + 2, 1) for k in (kin, kout)]
    ext = jnp.concatenate([jnp.where(ox, win, wout), ext, jnp.where(ox, wout, win)], axis=2)

    pitch = -(-(cols + 4) // 8) * 8
    depth = -(-((GROUP + 4) * pitch) // 128) * 128
    spread = np.zeros((32, depth), np.float32)
    for s in range(25):
        spread[s, (s // 5) * pitch + s % 5] = 1.0
    lanes = min(nv, 256)
    wide_rows = (rows - GROUP) * pitch + depth
    wide_rows = -(-max(wide_rows, (rows + 4) * pitch) // 16) * 16
    m = GROUP * cols
    fixed = lambda *s: pl.BlockSpec(s, lambda j: (0,) * len(s))
    flat_block = lambda n: pl.BlockSpec((n, lanes), lambda j: (0, j))
    edge_block = lambda n: pl.BlockSpec((n, 2, lanes), lambda j: (0, 0, j))
    normal, image = pl.pallas_call(
        image_kernel(rows, cols, pitch, depth),
        grid=(nv // lanes,),
        in_specs=[
            pl.BlockSpec(memory_space=pltpu.SMEM),
            fixed(9, rows + 2, cols + 2),
            fixed(32, depth),
            flat_block(rows * cols),
            flat_block(2 * cols),
            flat_block(2 * cols),
            edge_block(rows),
            edge_block(rows),
            edge_block(4),
            edge_block(4),
        ],
        out_specs=[fixed(25, rows, cols), flat_block(rows * cols)],
        out_shape=[
            jax.ShapeDtypeStruct((25, rows, cols), jnp.float32),
            jax.ShapeDtypeStruct((rows * cols, nv), jnp.float32),
        ],
        scratch_shapes=[
            pltpu.VMEM((rows // GROUP, 2 * m, depth), jnp.bfloat16),
            pltpu.VMEM((rows, 32, cols), jnp.float32),
            pltpu.VMEM((wide_rows, lanes), jnp.bfloat16),
            pltpu.VMEM((wide_rows, lanes), jnp.bfloat16),
        ],
        compiler_params=pltpu.CompilerParams(dimension_semantics=("arbitrary",)),
        name="image",
    )(
        jnp.stack([odd_y, odd_x]).astype(jnp.int32),
        ext,
        jnp.asarray(spread, jnp.bfloat16),
        vectors.reshape(rows * cols, nv),
        rin.reshape(2 * cols, nv),
        rout.reshape(2 * cols, nv),
        cin,
        cout,
        kin,
        kout,
    )
    return normal, image.reshape(rows, cols, nv)


def solution(mesh):
    in_specs = (P(None, "gy", "gx"), P("gy", "gx", None))
    out_specs = (P(None, "gy", "gx"), P("gy", "gx", None))
    return jax.shard_map(per_device, mesh=mesh, in_specs=in_specs, out_specs=out_specs, check_vma=False)
```

```python
import jax
import jax.numpy as jnp
import numpy as np
from jax import lax
from jax.experimental import pallas as pl
from jax.experimental.pallas import tpu as pltpu
from jax.sharding import PartitionSpec as P


GROUP = 2


def inner_swap(block, axis):
    n = lax.axis_size(axis)
    return lax.ppermute(block, axis, [(i, i ^ 1) for i in range(n) if i ^ 1 < n])


def outer_swap(block, axis):
    n = lax.axis_size(axis)
    partner = {i: ((i + 1) ^ 1) - 1 for i in range(n)}
    return lax.ppermute(block, axis, [(i, p) for i, p in partner.items() if 0 <= p < n])


def masked_weights(coefficients):
    _, rows, cols = coefficients.shape
    total_rows = rows * lax.axis_size("gy")
    total_cols = cols * lax.axis_size("gx")
    k = jnp.arange(9, dtype=jnp.int32)[:, None, None]
    r = lax.axis_index("gy") * rows + jnp.arange(rows, dtype=jnp.int32)[None, :, None] + k // 3 - 1
    c = lax.axis_index("gx") * cols + jnp.arange(cols, dtype=jnp.int32)[None, None, :] + k % 3 - 1
    inside = (r >= 0) & (r < total_rows) & (c >= 0) & (c < total_cols)
    return jnp.where(inside, coefficients, 0.0)


def normal_terms(ext_ref, rows, cols):
    acc = {}
    for k in range(9):
        a, b = k // 3 - 1, k % 3 - 1
        cells = [ext_ref[m, 1 - a : 1 - a + rows, 1 - b : 1 - b + cols] for m in range(9)]
        for m in range(9):
            slot = (m // 3 - k // 3 + 2) * 5 + (m % 3 - k % 3 + 2)
            product = cells[k] * cells[m]
            acc[slot] = acc[slot] + product if slot in acc else product
    return acc


def split(x):
    hi = x.astype(jnp.bfloat16)
    lo = (x - hi.astype(jnp.float32)).astype(jnp.bfloat16)
    return hi, lo


def weights_kernel(rows, cols, pitch):
    m = GROUP * cols

    def body(ext_ref, t_ref, n_ref, w_ref, n2_ref):
        for slot, term in normal_terms(ext_ref, rows, cols).items():
            n_ref[slot] = term
            n2_ref[:, slot, :] = term
        n2_ref[:, 25:, :] = jnp.zeros((rows, n2_ref.shape[1] - 25, cols), jnp.float32)
        dims = (((0,), (0,)), ((), ()))
        for r in range(rows):
            g, ro = divmod(r, GROUP)
            n_hi, n_lo = split(n2_ref[r])
            band = lax.dot_general(n_hi, t_ref[...], dims, preferred_element_type=jnp.float32) + lax.dot_general(
                n_lo, t_ref[...], dims, preferred_element_type=jnp.float32
            )
            band = pltpu.roll(band, ro * pitch, 1, stride=1, stride_axis=0)
            hi, lo = split(band)
            w_ref[g, ro * cols : (ro + 1) * cols, :] = hi
            w_ref[g, m + ro * cols : m + (ro + 1) * cols, :] = lo

    return body


def image_kernel(rows, cols, pitch, depth):
    m = GROUP * cols

    def body(odd_ref, w_ref, x_ref, rin_ref, rout_ref, cin_ref, cout_ref, kin_ref, kout_ref, out_ref, hi_ref, lo_ref):
        lanes = x_ref.shape[1]
        odd_y = odd_ref[0] == 1
        odd_x = odd_ref[1] == 1

        pad = jnp.zeros((pitch - cols - 4, lanes), jnp.float32)

        def sides(near_ref, far_ref, q):
            near, far = near_ref[q], far_ref[q]
            return jnp.where(odd_x, near, far), jnp.where(odd_x, far, near)

        def wide_row(i):
            if i < 2:
                at = slice(i * cols, (i + 1) * cols)
                mid = jnp.where(odd_y, rin_ref[at, :], rout_ref[at, :])
                l, r = sides(kin_ref, kout_ref, i)
            elif i < rows + 2:
                q = i - 2
                mid = x_ref[q * cols : (q + 1) * cols, :]
                l, r = sides(cin_ref, cout_ref, q)
            else:
                q = i - rows - 2
                at = slice(q * cols, (q + 1) * cols)
                mid = jnp.where(odd_y, rout_ref[at, :], rin_ref[at, :])
                l, r = sides(kin_ref, kout_ref, q + 2)
            return [l, mid, r, pad]

        for i in range(0, rows + 4, 2):
            pair = jnp.concatenate(wide_row(i) + wide_row(i + 1), axis=0)
            hi, lo = split(pair)
            hi_ref[i * pitch : (i + 2) * pitch, :] = hi
            lo_ref[i * pitch : (i + 2) * pitch, :] = lo
        tail = hi_ref.shape[0] - (rows + 4) * pitch
        if tail:
            hi_ref[(rows + 4) * pitch :, :] = jnp.zeros((tail, lanes), jnp.bfloat16)
            lo_ref[(rows + 4) * pitch :, :] = jnp.zeros((tail, lanes), jnp.bfloat16)
        for g in range(rows // GROUP):
            at = g * GROUP * pitch
            first = jnp.dot(w_ref[g], hi_ref[at : at + depth, :], preferred_element_type=jnp.float32)
            second = jnp.dot(w_ref[g, :m, :], lo_ref[at : at + depth, :], preferred_element_type=jnp.float32)
            out_ref[g * m : (g + 1) * m, :] = first[:m] + (first[m:] + second)

    return body


def edges(cells, odd, dim, width):
    size = cells.shape[dim]
    last = lax.slice_in_dim(cells, size - width, size, axis=dim)
    first = lax.slice_in_dim(cells, 0, width, axis=dim)
    return jnp.where(odd, first, last), jnp.where(odd, last, first)


def swapped(pair, axis):
    outer = outer_swap(pair[1], axis)
    return inner_swap(pair[0], axis), outer


def per_device(coefficients, vectors):
    _, rows, cols = coefficients.shape
    nv = vectors.shape[2]
    odd_y = lax.axis_index("gy") % 2
    odd_x = lax.axis_index("gx") % 2
    oy, ox = odd_y == 1, odd_x == 1
    col_pair = edges(vectors, ox, 1, 2)
    cin, cout = swapped(col_pair, "gx")
    *col_pair, vectors = lax.optimization_barrier((*col_pair, vectors))
    row_last = lax.dynamic_slice_in_dim(vectors, jnp.where(oy, 0, rows - 2), 2, axis=0)
    row_first = lax.dynamic_slice_in_dim(vectors, jnp.where(oy, rows - 2, 0), 2, axis=0)
    row_last, row_first, coefficients = lax.optimization_barrier((row_last, row_first, coefficients))
    rin, rout = swapped((row_last, row_first), "gy")
    masked = masked_weights(coefficients)
    pair = edges(masked, oy, 1, 1)
    min_, mout = swapped(pair, "gy")
    ext = jnp.concatenate([jnp.where(oy, min_, mout), masked, jnp.where(oy, mout, min_)], axis=1)
    win, wout = swapped(edges(ext, ox, 2, 1), "gx")
    ext = jnp.concatenate([jnp.where(ox, win, wout), ext, jnp.where(ox, wout, win)], axis=2)
    pitch = -(-(cols + 4) // 8) * 8
    depth = -(-((GROUP + 4) * pitch) // 128) * 128
    spread = np.zeros((32, depth), np.float32)
    for s in range(25):
        spread[s, (s // 5) * pitch + s % 5] = 1.0
    lanes = min(nv, 256)
    wide_rows = (rows - GROUP) * pitch + depth
    wide_rows = -(-max(wide_rows, (rows + 4) * pitch) // 16) * 16
    m = GROUP * cols
    fixed = lambda *s: pl.BlockSpec(s, lambda j: (0,) * len(s))
    flat_block = lambda n: pl.BlockSpec((n, lanes), lambda j: (0, j))
    edge_block = lambda n: pl.BlockSpec((n, 2, lanes), lambda j: (0, 0, j))
    whole = pl.BlockSpec(memory_space=pltpu.VMEM)
    normal, banded = pl.pallas_call(
        weights_kernel(rows, cols, pitch),
        in_specs=[whole, whole],
        out_specs=[whole, whole],
        out_shape=[
            jax.ShapeDtypeStruct((25, rows, cols), jnp.float32),
            jax.ShapeDtypeStruct((rows // GROUP, 2 * m, depth), jnp.bfloat16),
        ],
        scratch_shapes=[pltpu.VMEM((rows, 32, cols), jnp.float32)],
        name="weights",
    )(ext, jnp.asarray(spread, jnp.bfloat16))
    rin, rout, banded = lax.optimization_barrier((rin, rout, banded))
    corner = []
    for vin, vout in zip(edges(rin, ox, 1, 2), edges(rout, ox, 1, 2)):
        corner.append(jnp.concatenate([jnp.where(oy, vin, vout), jnp.where(oy, vout, vin)], axis=0))
    kin, kout = swapped(corner, "gx")

    image = pl.pallas_call(
        image_kernel(rows, cols, pitch, depth),
        grid=(nv // lanes,),
        in_specs=[
            pl.BlockSpec(memory_space=pltpu.SMEM),
            fixed(rows // GROUP, 2 * m, depth),
            flat_block(rows * cols),
            flat_block(2 * cols),
            flat_block(2 * cols),
            edge_block(rows),
            edge_block(rows),
            edge_block(4),
            edge_block(4),
        ],
        out_specs=flat_block(rows * cols),
        out_shape=jax.ShapeDtypeStruct((rows * cols, nv), jnp.float32),
        scratch_shapes=[
            pltpu.VMEM((wide_rows, lanes), jnp.bfloat16),
            pltpu.VMEM((wide_rows, lanes), jnp.bfloat16),
        ],
        compiler_params=pltpu.CompilerParams(dimension_semantics=("arbitrary",)),
        name="image",
    )(
        jnp.stack([odd_y, odd_x]).astype(jnp.int32),
        banded,
        vectors.reshape(rows * cols, nv),
        rin.reshape(2 * cols, nv),
        rout.reshape(2 * cols, nv),
        cin,
        cout,
        kin,
        kout,
    )
    return normal, image.reshape(rows, cols, nv)


def solution(mesh):
    in_specs = (P(None, "gy", "gx"), P("gy", "gx", None))
    out_specs = (P(None, "gy", "gx"), P("gy", "gx", None))

    return jax.shard_map(per_device, mesh=mesh, in_specs=in_specs, out_specs=out_specs, check_vma=False)
```

```python
import jax
import jax.numpy as jnp
import numpy as np
from jax import lax
from jax.experimental import pallas as pl
from jax.experimental.pallas import tpu as pltpu
from jax.sharding import PartitionSpec as P


GROUP = 2
STRIPS = 4


def inner_swap(block, axis):
    n = lax.axis_size(axis)
    return lax.ppermute(block, axis, [(i, i ^ 1) for i in range(n) if i ^ 1 < n])


def outer_swap(block, axis):
    n = lax.axis_size(axis)
    partner = {i: ((i + 1) ^ 1) - 1 for i in range(n)}
    return lax.ppermute(block, axis, [(i, p) for i, p in partner.items() if 0 <= p < n])


def masked_weights(coefficients):
    _, rows, cols = coefficients.shape
    total_rows = rows * lax.axis_size("gy")
    total_cols = cols * lax.axis_size("gx")
    k = jnp.arange(9, dtype=jnp.int32)[:, None, None]
    r = lax.axis_index("gy") * rows + jnp.arange(rows, dtype=jnp.int32)[None, :, None] + k // 3 - 1
    c = lax.axis_index("gx") * cols + jnp.arange(cols, dtype=jnp.int32)[None, None, :] + k % 3 - 1
    inside = (r >= 0) & (r < total_rows) & (c >= 0) & (c < total_cols)
    return jnp.where(inside, coefficients, 0.0)


def normal_terms(ext_ref, rows, cols):
    acc = {}
    for k in range(9):
        a, b = k // 3 - 1, k % 3 - 1
        cells = [ext_ref[m, 1 - a : 1 - a + rows, 1 - b : 1 - b + cols] for m in range(9)]
        for m in range(9):
            slot = (m // 3 - k // 3 + 2) * 5 + (m % 3 - k % 3 + 2)
            product = cells[k] * cells[m]
            acc[slot] = acc[slot] + product if slot in acc else product
    return acc


def split(x):
    hi = x.astype(jnp.bfloat16)
    lo = (x - hi.astype(jnp.float32)).astype(jnp.bfloat16)
    return hi, lo


def weights_kernel(rows, cols, pitch):
    m = GROUP * cols

    def body(ext_ref, t_ref, n_ref, w_ref, n2_ref):
        for slot, term in normal_terms(ext_ref, rows, cols).items():
            n_ref[slot] = term
            n2_ref[:, slot, :] = term
        n2_ref[:, 25:, :] = jnp.zeros((rows, n2_ref.shape[1] - 25, cols), jnp.float32)
        dims = (((0,), (0,)), ((), ()))
        for r in range(rows):
            g, ro = divmod(r, GROUP)
            n_hi, n_lo = split(n2_ref[r])
            band = lax.dot_general(n_hi, t_ref[...], dims, preferred_element_type=jnp.float32) + lax.dot_general(
                n_lo, t_ref[...], dims, preferred_element_type=jnp.float32
            )
            band = pltpu.roll(band, ro * pitch, 1, stride=1, stride_axis=0)
            hi, lo = split(band)
            w_ref[g, ro * cols : (ro + 1) * cols, :] = hi
            w_ref[g, m + ro * cols : m + (ro + 1) * cols, :] = lo

    return body


def image_kernel(rows, cols, pitch, depth):
    m = GROUP * cols

    def body(odd_ref, w_ref, *refs):
        x_refs = refs[:STRIPS]
        rin_ref, rout_ref, cin_ref, cout_ref, kin_ref, kout_ref, out_ref, hi_ref, lo_ref = refs[STRIPS:]
        lanes = out_ref.shape[1]
        strip = rows // STRIPS
        odd_y = odd_ref[0] == 1
        odd_x = odd_ref[1] == 1

        pad = jnp.zeros((pitch - cols - 4, lanes), jnp.float32)

        def sides(near_ref, far_ref, q):
            near, far = near_ref[q], far_ref[q]
            return jnp.where(odd_x, near, far), jnp.where(odd_x, far, near)

        def wide_row(i):
            if i < 2:
                at = slice(i * cols, (i + 1) * cols)
                mid = jnp.where(odd_y, rin_ref[at, :], rout_ref[at, :])
                l, r = sides(kin_ref, kout_ref, i)
            elif i < rows + 2:
                q = i - 2
                mid = x_refs[q // strip][q % strip * cols : (q % strip + 1) * cols, :]
                l, r = sides(cin_ref, cout_ref, q)
            else:
                q = i - rows - 2
                at = slice(q * cols, (q + 1) * cols)
                mid = jnp.where(odd_y, rout_ref[at, :], rin_ref[at, :])
                l, r = sides(kin_ref, kout_ref, q + 2)
            return [l, mid, r, pad]

        for i in range(0, rows + 4, 2):
            pair = jnp.concatenate(wide_row(i) + wide_row(i + 1), axis=0)
            hi, lo = split(pair)
            hi_ref[i * pitch : (i + 2) * pitch, :] = hi
            lo_ref[i * pitch : (i + 2) * pitch, :] = lo
        tail = hi_ref.shape[0] - (rows + 4) * pitch
        if tail:
            hi_ref[(rows + 4) * pitch :, :] = jnp.zeros((tail, lanes), jnp.bfloat16)
            lo_ref[(rows + 4) * pitch :, :] = jnp.zeros((tail, lanes), jnp.bfloat16)
        for g in range(rows // GROUP):
            at = g * GROUP * pitch
            first = jnp.dot(w_ref[g], hi_ref[at : at + depth, :], preferred_element_type=jnp.float32)
            second = jnp.dot(w_ref[g, :m, :], lo_ref[at : at + depth, :], preferred_element_type=jnp.float32)
            out_ref[g * m : (g + 1) * m, :] = first[:m] + (first[m:] + second)

    return body


def edges(cells, odd, dim, width):
    size = cells.shape[dim]
    last = lax.slice_in_dim(cells, size - width, size, axis=dim)
    first = lax.slice_in_dim(cells, 0, width, axis=dim)
    return jnp.where(odd, first, last), jnp.where(odd, last, first)


def swapped(pair, axis):
    outer = outer_swap(pair[1], axis)
    return inner_swap(pair[0], axis), outer


def per_device(coefficients, vectors):
    _, rows, cols = coefficients.shape
    nv = vectors.shape[2]
    odd_y = lax.axis_index("gy") % 2
    odd_x = lax.axis_index("gx") % 2
    oy, ox = odd_y == 1, odd_x == 1
    masked = masked_weights(coefficients)
    pair = edges(masked, oy, 1, 1)
    min_, mout = swapped(pair, "gy")
    ext = jnp.concatenate([jnp.where(oy, min_, mout), masked, jnp.where(oy, mout, min_)], axis=1)
    pair = edges(ext, ox, 2, 1)
    win, wout = swapped(pair, "gx")
    ext = jnp.concatenate([jnp.where(ox, win, wout), ext, jnp.where(ox, wout, win)], axis=2)
    col_pair = edges(vectors, ox, 1, 2)
    cin, cout = swapped(col_pair, "gx")
    row_last = lax.dynamic_slice_in_dim(vectors, jnp.where(oy, 0, rows - 2), 2, axis=0)
    row_first = lax.dynamic_slice_in_dim(vectors, jnp.where(oy, rows - 2, 0), 2, axis=0)
    rin, rout = swapped((row_last, row_first), "gy")

    pitch = -(-(cols + 4) // 8) * 8
    depth = -(-((GROUP + 4) * pitch) // 128) * 128
    spread = np.zeros((32, depth), np.float32)
    for s in range(25):
        spread[s, (s // 5) * pitch + s % 5] = 1.0
    lanes = min(nv, 256)
    wide_rows = (rows - GROUP) * pitch + depth
    wide_rows = -(-max(wide_rows, (rows + 4) * pitch) // 16) * 16
    m = GROUP * cols
    fixed = lambda *s: pl.BlockSpec(s, lambda j: (0,) * len(s))
    flat_block = lambda n: pl.BlockSpec((n, lanes), lambda j: (0, j))
    edge_block = lambda n: pl.BlockSpec((n, 2, lanes), lambda j: (0, 0, j))
    whole = pl.BlockSpec(memory_space=pltpu.VMEM)
    normal, banded = pl.pallas_call(
        weights_kernel(rows, cols, pitch),
        in_specs=[whole, whole],
        out_specs=[whole, whole],
        out_shape=[
            jax.ShapeDtypeStruct((25, rows, cols), jnp.float32),
            jax.ShapeDtypeStruct((rows // GROUP, 2 * m, depth), jnp.bfloat16),
        ],
        scratch_shapes=[pltpu.VMEM((rows, 32, cols), jnp.float32)],
        name="weights",
    )(ext, jnp.asarray(spread, jnp.bfloat16))
    rin, rout, banded = lax.optimization_barrier((rin, rout, banded))
    corner = []
    for vin, vout in zip(edges(rin, ox, 1, 2), edges(rout, ox, 1, 2)):
        corner.append(jnp.concatenate([jnp.where(oy, vin, vout), jnp.where(oy, vout, vin)], axis=0))
    kin, kout = swapped(corner, "gx")

    image = pl.pallas_call(
        image_kernel(rows, cols, pitch, depth),
        grid=(nv // lanes,),
        in_specs=[
            pl.BlockSpec(memory_space=pltpu.SMEM),
            fixed(rows // GROUP, 2 * m, depth),
            *[pl.BlockSpec((rows // STRIPS * cols, lanes), lambda j, q=q: (q, j)) for q in range(STRIPS)],
            flat_block(2 * cols),
            flat_block(2 * cols),
            edge_block(rows),
            edge_block(rows),
            edge_block(4),
            edge_block(4),
        ],
        out_specs=flat_block(rows * cols),
        out_shape=jax.ShapeDtypeStruct((rows * cols, nv), jnp.float32),
        scratch_shapes=[
            pltpu.VMEM((wide_rows, lanes), jnp.bfloat16),
            pltpu.VMEM((wide_rows, lanes), jnp.bfloat16),
        ],
        compiler_params=pltpu.CompilerParams(dimension_semantics=("arbitrary",)),
        name="image",
    )(
        jnp.stack([odd_y, odd_x]).astype(jnp.int32),
        banded,
        *[vectors.reshape(rows * cols, nv)] * STRIPS,
        rin.reshape(2 * cols, nv),
        rout.reshape(2 * cols, nv),
        cin,
        cout,
        kin,
        kout,
    )
    return normal, image.reshape(rows, cols, nv)


def solution(mesh):
    in_specs = (P(None, "gy", "gx"), P("gy", "gx", None))
    out_specs = (P(None, "gy", "gx"), P("gy", "gx", None))

    return jax.shard_map(per_device, mesh=mesh, in_specs=in_specs, out_specs=out_specs, check_vma=False)
```
